32 devices in a mesh: rep: 4 (over x, y), dp: 8 (over z, core).
Axes of the slice: x: 2, y: 2, z: 4, core: 2. Of those that a mesh axis runs over, the one named last changes fastest.
Arguments:
- g_w_gate: bfloat16 [32, 2, 512, 8192], P(('rep', 'dp')), parts along dimension 0
- g_w_up: bfloat16 [32, 2, 512, 8192], P(('rep', 'dp')), parts along dimension 0
- g_w_down: bfloat16 [32, 2, 8192, 512], P(('rep', 'dp')), parts along dimension 0
- w_gate: bfloat16 [2, 512, 8192], replicated
- w_up: bfloat16 [2, 512, 8192], replicated
- w_down: bfloat16 [2, 8192, 512], replicated
- m_w_gate: float32 [2, 512, 8192], P(None, 'dp')
- m_w_up: float32 [2, 512, 8192], P(None, 'dp')
- m_w_down: float32 [2, 8192, 512], P(None, 'dp')
- v_w_gate: float32 [2, 512, 8192], P(None, 'dp')
- v_w_up: float32 [2, 512, 8192], P(None, 'dp')
- v_w_down: float32 [2, 8192, 512], P(None, 'dp')
Outputs:
- output 1: bfloat16 [8, 512, 8192], P('rep'), parts along dimension 0
- output 2: bfloat16 [8, 512, 8192], P('rep'), parts along dimension 0
- output 3: bfloat16 [8, 8192, 512], P('rep'), parts along dimension 0
- output 4: float32 [8, 512, 8192], P('rep', 'dp'), parts along dimension 0
- output 5: float32 [8, 512, 8192], P('rep', 'dp'), parts along dimension 0
- output 6: float32 [8, 8192, 512], P('rep', 'dp'), parts along dimension 0
- output 7: float32 [8, 512, 8192], P('rep', 'dp'), parts along dimension 0
- output 8: float32 [8, 512, 8192], P('rep', 'dp'), parts along dimension 0
- output 9: float32 [8, 8192, 512], P('rep', 'dp'), parts along dimension 0
There are 4 independent parts. The reference program is written for one: setup_inputs(seed, part) draws one part's arguments, and reference() takes and returns one part's arrays. A program takes and returns all parts, laid end to end along the dimension named above; an argument that names none is the same for every part.
All inputs are finite; a program needn't handle non-finite values.
Results may differ from the reference program's by a relative error of at most 0.022.
Values are sent between devices in bfloat16 or wider.
A program may use at most 2 GiB of HBM per device.

```python
import jax
import jax.numpy as jnp
from jax import lax

DEVICES = 8
D = 512
FF = 8192
LAYERS = 2
NAMES = ("w_gate", "w_up", "w_down")
SHAPES = {"w_gate": (LAYERS, D, FF), "w_up": (LAYERS, D, FF), "w_down": (LAYERS, FF, D)}


def setup_inputs(seed: int = 0, part: int = 0) -> dict:
    kz, *keys = jax.random.split(jax.random.key(seed), 1 + 5 * len(NAMES))
    loud = 2.0 ** jax.random.uniform(kz, (), jnp.float32, -1.0, 1.0)
    drawn = {}
    for name, key, both in zip(NAMES, keys[:3], keys[3:6], strict=True):
        own = jax.random.normal(jax.random.fold_in(key, part), (DEVICES, *SHAPES[name]), jnp.float32)
        shared = jax.random.normal(jax.random.fold_in(both, part), SHAPES[name], jnp.float32)
        drawn["g_" + name] = (loud * (0.7 * shared / DEVICES + 0.7 * own * DEVICES**-0.5)).astype(jnp.bfloat16)
    for name, key in zip(NAMES, keys[6:9], strict=True):
        drawn[name] = (jax.random.normal(key, SHAPES[name], jnp.float32) * SHAPES[name][1] ** -0.5).astype(jnp.bfloat16)
    for name, key in zip(NAMES, keys[9:12], strict=True):
        drawn["m_" + name] = loud * 0.5 * jax.random.normal(key, SHAPES[name], jnp.float32)
    for name, key in zip(NAMES, keys[12:15], strict=True):
        drawn["v_" + name] = loud * loud * jax.random.uniform(key, SHAPES[name], jnp.float32, 0.5, 1.5)
    return drawn


def adamw(w, m, v, g):
    m = 0.9 * m + 0.1 * g
    v = 0.95 * v + 0.05 * g * g
    step = m * lax.rsqrt(v + 1e-8) + 0.1 * w
    return (w - 0.02 * step).astype(jnp.bfloat16), m, v


def reference(g_w_gate, g_w_up, g_w_down, w_gate, w_up, w_down, m_w_gate, m_w_up, m_w_down, v_w_gate, v_w_up, v_w_down):
    def total(terms):
        return lax.scan(lambda so_far, term: (so_far + term.astype(jnp.float32), None), jnp.zeros(terms.shape[1:], jnp.float32), terms)[0]

    gradients = [total(terms).astype(jnp.bfloat16).astype(jnp.float32) for terms in (g_w_gate, g_w_up, g_w_down)]
    new = [
        adamw(w.astype(jnp.float32), m, v, g)
        for w, m, v, g in zip((w_gate, w_up, w_down), (m_w_gate, m_w_up, m_w_down), (v_w_gate, v_w_up, v_w_down), gradients, strict=True)
    ]
    return tuple(one[which] for which in range(3) for one in new)
```

```python
import functools

import jax
import jax.numpy as jnp
from jax import lax
from jax.experimental import pallas as pl
from jax.experimental.pallas import tpu as pltpu
from jax.sharding import PartitionSpec as P

MESH = pl.DeviceIdType.MESH
CHIPS = 4
LAG = 2
AHEAD = 3
OWN, PAR, ARR, SND, MOM, NEW, GAT = 3, 4, 4, 3, 3, 3, 4
PIECES = 32
SHAPES = ((16, 2048), (16, 2048), (64, 512))


def adamw(w, m, v, g):
    m = 0.9 * m + 0.1 * g
    v = 0.95 * v + 0.05 * g * g
    step = m * lax.rsqrt(v + 1e-8) + 0.1 * w
    return (w - 0.02 * step).astype(jnp.bfloat16), m, v


def piece(ref, w, block, q):
    layer, at = lax.div(q, 16), lax.rem(q, 16)
    if w < 2:
        row = pl.multiple_of(block * 64 + lax.div(at, 4) * 16, 16)
        return ref.at[layer, pl.ds(row, 16), pl.ds(pl.multiple_of(lax.rem(at, 4) * 2048, 2048), 2048)]
    return ref.at[layer, pl.ds(pl.multiple_of(block * 1024 + at * 64, 64), 64), :]


def chunks(w):
    rows, columns = SHAPES[w]
    for r in range(0, rows, 16):
        for c in range(0, columns, 512):
            yield pl.ds(r, 16), pl.ds(c, 512)


def owned_lag(z):
    return LAG * max(z, CHIPS - 1 - z)


def gather_lag(owner, z):
    return owned_lag(owner) + LAG * abs(owner - z)


def kernel(*refs):
    terms, weights, m_in, v_in = (refs[i : i + 3] for i in (0, 3, 6, 9))
    whole, m_out, v_out = (refs[i : i + 3] for i in (12, 15, 18))
    (own_a, own_b, par_a, par_b, arr_a, arr_b, snd_a, snd_b, m_a, m_b, v_a, v_b, w_a, w_b, mo_a, mo_b, vo_a, vo_b, new_a, new_b) = refs[21:41]
    (own_sem, par_recv, par_send, arr_sem, snd_sem, m_sem, v_sem, w_sem, mo_sem, vo_sem, new_sem, gat_recv, gat_send, pal_send, pal_recv) = refs[41:]

    me = lax.axis_index("dp")
    core = lax.rem(me, 2)
    chip = lax.div(me, 2)
    partner = me + 1 - 2 * core

    def slot(a, b, w, n, *lead):
        return a.at[(*lead, w, n)] if w < 2 else b.at[(*lead, n)]

    def remote(src, dst, send, recv, to):
        return pltpu.make_async_remote_copy(src_ref=src, dst_ref=dst, send_sem=send, recv_sem=recv, device_id={"dp": to}, device_id_type=MESH)

    def body(z):
        left, right = z > 0, z < CHIPS - 1
        others = sorted((o for o in range(CHIPS) if o != z), key=lambda o: -abs(o - z))
        neighbours = [partner] + ([me - 2] if left else []) + ([me + 2] if right else [])

        def upstream(o):
            return left if o > z else right

        for o in others:
            if not upstream(o):
                arr_a[o] = jnp.zeros_like(arr_a[o])
                arr_b[o] = jnp.zeros_like(arr_b[o])
        for o, there in ((z, left), (CHIPS, right)):
            if not there:
                arr_a[o] = jnp.zeros_like(arr_a[o])
                arr_b[o] = jnp.zeros_like(arr_b[o])

        barrier = pltpu.get_barrier_semaphore()
        for other in neighbours:
            pl.semaphore_signal(barrier, inc=1, device_id={"dp": other}, device_id_type=MESH)
        pl.semaphore_wait(barrier, len(neighbours))

        def lag(o):
            return owned_lag(z) if o == z else LAG * (z if o > z else CHIPS - 1 - z)

        def own_copy(w, q, o):
            n = lax.rem(q, OWN)
            return pltpu.make_async_copy(piece(terms[w], w, 2 * o + core, q), slot(own_a, own_b, w, n, o), own_sem.at[o, w, n])

        def par_copy(w, q, o):
            n = lax.rem(q, PAR)
            return remote(piece(terms[w], w, 2 * o + 1 - core, q), slot(par_a, par_b, w, n, o), par_send.at[o, w, n], par_recv.at[o, w, n], partner)

        def sum_copy(w, q, o):
            n, k = lax.rem(q, SND), lax.rem(q, ARR)
            way = 1 if o > z else -1
            there = CHIPS if way < 0 and o == z - 1 else o
            return remote(slot(snd_a, snd_b, w, n, o), slot(arr_a, arr_b, w, k, there), snd_sem.at[o, w, n], arr_sem.at[there, w, k], me + 2 * way)

        def arr_wait(w, q, o):
            k = lax.rem(q, ARR)
            there = slot(arr_a, arr_b, w, k, o)
            remote(there, there, snd_sem.at[0, w, 0], arr_sem.at[o, w, k], me).wait_recv()

        def state_copies(w, q):
            n = lax.rem(q, MOM)
            return (
                pltpu.make_async_copy(piece(m_in[w], w, 0, q), slot(m_a, m_b, w, n), m_sem.at[w, n]),
                pltpu.make_async_copy(piece(v_in[w], w, 0, q), slot(v_a, v_b, w, n), v_sem.at[w, n]),
                pltpu.make_async_copy(piece(weights[w], w, me, q), slot(w_a, w_b, w, n), w_sem.at[w, n]),
            )

        def result_copies(w, q):
            n, k = lax.rem(q, NEW), lax.rem(q, GAT)
            new, there = slot(new_a, new_b, w, n), piece(whole[w], w, me, q)
            local = [
                pltpu.make_async_copy(slot(mo_a, mo_b, w, n), piece(m_out[w], w, 0, q), mo_sem.at[w, n]),
                pltpu.make_async_copy(slot(vo_a, vo_b, w, n), piece(v_out[w], w, 0, q), vo_sem.at[w, n]),
                pltpu.make_async_copy(new, there, new_sem.at[0, w, n]),
            ]
            far = [remote(new, there, new_sem.at[1, w, n], gat_recv.at[z, w, k], me + 2)] if right else []
            far += [remote(new, there, new_sem.at[2, w, n], gat_recv.at[z, w, k], me - 2)] if left else []
            far += [remote(new, there, new_sem.at[3, w, n], pal_recv.at[w], partner)]
            return local, far

        def pass_copies(w, q, o):
            k = lax.rem(q, GAT)
            there = piece(whole[w], w, 2 * o + core, q)
            way = -1 if o > z else 1
            on = left if o > z else right
            far = [remote(there, there, gat_send.at[o, w, k], gat_recv.at[o, w, k], me + 2 * way)] if on else []
            return far + [remote(there, there, pal_send.at[o, w, k], pal_recv.at[w], partner)]

        def pass_wait(w, q, o):
            k = lax.rem(q, GAT)
            there = piece(whole[w], w, 2 * o + core, q)
            remote(there, there, gat_send.at[o, w, k], gat_recv.at[o, w, k], me).wait_recv()

        def at(i, k, lag):
            w = (k - lag) % 3
            return w, i + (k - lag - w) // 3

        def valid(q):
            return (q >= 0) & (q < PIECES)

        def fetch(i, k):
            for o in (*others, z):
                w, q = at(i, k, lag(o) - AHEAD)

                @pl.when(valid(q))
                def _(w=w, q=q, o=o):
                    @pl.when(q >= PAR)
                    def _():
                        par_copy(w, q - PAR, o).wait_send()

                    par_copy(w, q, o).start()
                    own_copy(w, q, o).start()
                    if o == z:
                        for copy in state_copies(w, q):
                            copy.start()

        def forward(i, k, o):
            w, q = at(i, k, lag(o))

            @pl.when(valid(q))
            def _():
                own_copy(w, q, o).wait()
                par_copy(w, q, o).wait_recv()
                if upstream(o):
                    arr_wait(w, q, o)

                @pl.when(q >= SND)
                def _():
                    sum_copy(w, q - SND, o).wait_send()

                own, par = slot(own_a, own_b, w, lax.rem(q, OWN), o), slot(par_a, par_b, w, lax.rem(q, PAR), o)
                arr, snd = slot(arr_a, arr_b, w, lax.rem(q, ARR), o), slot(snd_a, snd_b, w, lax.rem(q, SND), o)
                for r, c in chunks(w):
                    total = own[r, c].astype(jnp.float32) + par[r, c].astype(jnp.float32) + arr[r, c].astype(jnp.float32)
                    snd[r, c] = total.astype(jnp.bfloat16)
                sum_copy(w, q, o).start()

        def finish(i, k):
            w, q = at(i, k, lag(z))

            @pl.when(valid(q))
            def _():
                own_copy(w, q, z).wait()
                par_copy(w, q, z).wait_recv()
                for copy in state_copies(w, q):
                    copy.wait()
                if left:
                    arr_wait(w, q, z)
                if right:
                    arr_wait(w, q, CHIPS)

                @pl.when(q >= NEW)
                def _():
                    drain_result(w, q - NEW)

                own, par = slot(own_a, own_b, w, lax.rem(q, OWN), z), slot(par_a, par_b, w, lax.rem(q, PAR), z)
                one, two = slot(arr_a, arr_b, w, lax.rem(q, ARR), z), slot(arr_a, arr_b, w, lax.rem(q, ARR), CHIPS)
                n, k = lax.rem(q, MOM), lax.rem(q, NEW)
                m, v, old = slot(m_a, m_b, w, n), slot(v_a, v_b, w, n), slot(w_a, w_b, w, n)
                mo, vo, new = slot(mo_a, mo_b, w, k), slot(vo_a, vo_b, w, k), slot(new_a, new_b, w, k)
                for r, c in chunks(w):
                    total = own[r, c].astype(jnp.float32) + par[r, c].astype(jnp.float32)
                    total = total + one[r, c].astype(jnp.float32) + two[r, c].astype(jnp.float32)
                    g = total.astype(jnp.bfloat16).astype(jnp.float32)
                    new[r, c], mo[r, c], vo[r, c] = adamw(old[r, c].astype(jnp.float32), m[r, c], v[r, c], g)
                local, far = result_copies(w, q)
                for copy in (*far, *local):
                    copy.start()

        def drain_result(w, q):
            local, far = result_copies(w, q)
            for copy in local:
                copy.wait()
            for copy in far:
                copy.wait_send()

        def pass_on(i, k, o):
            w, q = at(i, k, gather_lag(o, z))

            @pl.when(valid(q))
            def _():
                pass_wait(w, q, o)

                @pl.when(q >= GAT)
                def _():
                    for copy in pass_copies(w, q - GAT, o):
                        copy.wait_send()

                for copy in pass_copies(w, q, o):
                    copy.start()

        last = 3 * PIECES + max(gather_lag(o, z) for o in range(CHIPS))

        @pl.loop(-(AHEAD // 3), -(-last // 3))
        def _(i):
            for k in range(3):
                fetch(i, k)
                for o in others:
                    forward(i, k, o)
                finish(i, k)
                for o in others:
                    pass_on(i, k, o)

        def tail(ring, wait):
            @pl.loop(PIECES - ring, PIECES)
            def _(q):
                for w in range(3):
                    wait(w, q)

        def tail_par(w, q):
            for o in range(CHIPS):
                par_copy(w, q, o).wait_send()

        def tail_sum(w, q):
            for o in others:
                sum_copy(w, q, o).wait_send()

        def tail_pass(w, q):
            for o in others:
                for copy in pass_copies(w, q, o):
                    copy.wait_send()

        tail(PAR, tail_par)
        tail(SND, tail_sum)
        tail(NEW, drain_result)
        tail(GAT, tail_pass)
        for w in range(3):
            half = whole[w].at[0]
            pltpu.make_async_copy(half, half, pal_recv.at[w]).wait()

    for z in range(CHIPS):

        @pl.when(chip == z)
        def _(z=z):
            body(z)


def communicate(terms, weights, m, v):
    def ring(dtype, *lead):
        return [pltpu.VMEM((*lead[:-1], 2, lead[-1], *SHAPES[0]), dtype), pltpu.VMEM((*lead, *SHAPES[2]), dtype)]

    dma = pltpu.SemaphoreType.DMA
    bf16, f32 = jnp.bfloat16, jnp.float32
    return pl.pallas_call(
        kernel,
        out_shape=[jax.ShapeDtypeStruct(a.shape, a.dtype) for a in (*weights, *m, *v)],
        in_specs=[pl.BlockSpec(memory_space=pl.ANY)] * 12,
        out_specs=[pl.BlockSpec(memory_space=pl.ANY)] * 9,
        scratch_shapes=[
            *ring(bf16, CHIPS, OWN),
            *ring(bf16, CHIPS, PAR),
            *ring(bf16, CHIPS + 1, ARR),
            *ring(bf16, CHIPS, SND),
            *ring(f32, MOM),
            *ring(f32, MOM),
            *ring(bf16, MOM),
            *ring(f32, NEW),
            *ring(f32, NEW),
            *ring(bf16, NEW),
            dma((CHIPS, 3, OWN)),
            dma((CHIPS, 3, PAR)),
            dma((CHIPS, 3, PAR)),
            dma((CHIPS + 1, 3, ARR)),
            dma((CHIPS, 3, SND)),
            dma((3, MOM)),
            dma((3, MOM)),
            dma((3, MOM)),
            dma((3, NEW)),
            dma((3, NEW)),
            dma((4, 3, NEW)),
            dma((CHIPS, 3, GAT)),
            dma((CHIPS, 3, GAT)),
            dma((CHIPS, 3, GAT)),
            dma((3,)),
        ],
        compiler_params=pltpu.CompilerParams(collective_id=0, has_side_effects=True),
        name="sum_step_gather",
    )(*terms, *weights, *m, *v)


def hand_out(arrays):
    steps = 16

    def spec(a):
        _, rows, columns = a.shape
        return pl.BlockSpec((1, rows * 2 // steps, columns), lambda i: (lax.div(i, steps // 2), lax.rem(i, steps // 2), 0))

    def copy(*refs):
        for i, o in zip(refs[:9], refs[9:], strict=True):
            o[...] = i[...]

    return pl.pallas_call(
        copy,
        grid=(steps,),
        out_shape=[jax.ShapeDtypeStruct(a.shape, a.dtype) for a in arrays],
        in_specs=[spec(a) for a in arrays],
        out_specs=[spec(a) for a in arrays],
        name="hand_out",
    )(*arrays)


def solution(mesh):
    def step(*arrays):
        terms, weights, m, v = (arrays[i : i + 3] for i in (0, 3, 6, 9))
        terms = [t.reshape(t.shape[1:]) for t in terms]
        return tuple(hand_out(communicate(terms, weights, m, v)))

    all_of, cut = P(None, None, None), P(None, "dp", None)
    return jax.shard_map(
        step,
        mesh=mesh,
        in_specs=(P(("rep", "dp"), None, None, None),) * 3 + (all_of,) * 3 + (cut,) * 6,
        out_specs=(P("rep", None, None),) * 3 + (P("rep", "dp", None),) * 6,
        check_vma=False,
    )
```

```python
import functools

import jax
import jax.numpy as jnp
from jax import lax
from jax.experimental import pallas as pl
from jax.experimental.pallas import tpu as pltpu
from jax.sharding import PartitionSpec as P

MESH = pl.DeviceIdType.MESH
CHIPS = 4
LIMIT = 14 << 20
LAG = 1
AHEAD = 3
OWN, PAR, ARR, SND, MOM, NEW, GAT = 2, 3, 3, 2, 2, 2, 4
PIECES = 32
SHAPES = ((16, 2048), (16, 2048), (64, 512))


def adamw(w, m, v, g):
    m = 0.9 * m + 0.1 * g
    v = 0.95 * v + 0.05 * g * g
    step = m * lax.rsqrt(v + 1e-8) + 0.1 * w
    return (w - 0.02 * step).astype(jnp.bfloat16), m, v


def piece(ref, w, block, q):
    layer, at = lax.div(q, 16), lax.rem(q, 16)
    if w < 2:
        row = pl.multiple_of(block * 64 + lax.div(at, 4) * 16, 16)
        return ref.at[layer, pl.ds(row, 16), pl.ds(pl.multiple_of(lax.rem(at, 4) * 2048, 2048), 2048)]
    return ref.at[layer, pl.ds(pl.multiple_of(block * 1024 + at * 64, 64), 64), :]


def chunks(w):
    rows, columns = SHAPES[w]
    for r in range(0, rows, 16):
        for c in range(0, columns, 512):
            yield pl.ds(r, 16), pl.ds(c, 512)


def owned_lag(z):
    return LAG * max(z, CHIPS - 1 - z)


def gather_lag(owner, z):
    return owned_lag(owner) + LAG * abs(owner - z)


def kernel(*refs):
    terms, weights, m_in, v_in = (refs[i : i + 3] for i in (0, 3, 6, 9))
    whole, m_out, v_out = (refs[i : i + 3] for i in (12, 15, 18))
    (own_a, own_b, par_a, par_b, arr_a, arr_b, snd_a, snd_b, m_a, m_b, v_a, v_b, w_a, w_b, mo_a, mo_b, vo_a, vo_b) = refs[21:39]
    (own_sem, par_recv, par_send, arr_sem, snd_sem, m_sem, v_sem, w_sem, mo_sem, vo_sem, new_sem, gat_recv, gat_send, pal_send, pal_recv) = refs[39:]

    me = lax.axis_index("dp")
    core = lax.rem(me, 2)
    chip = lax.div(me, 2)
    partner = me + 1 - 2 * core

    def slot(a, b, w, n, *lead):
        return a.at[(*lead, w, n)] if w < 2 else b.at[(*lead, n)]

    def remote(src, dst, send, recv, to):
        return pltpu.make_async_remote_copy(src_ref=src, dst_ref=dst, send_sem=send, recv_sem=recv, device_id={"dp": to}, device_id_type=MESH)

    def body(z):
        left, right = z > 0, z < CHIPS - 1
        others = sorted((o for o in range(CHIPS) if o != z), key=lambda o: -abs(o - z))
        neighbours = [partner] + ([me - 2] if left else []) + ([me + 2] if right else [])

        def upstream(o):
            return left if o > z else right

        for o in others:
            if not upstream(o):
                arr_a[o] = jnp.zeros_like(arr_a[o])
                arr_b[o] = jnp.zeros_like(arr_b[o])
        for o, there in ((z, left), (CHIPS, right)):
            if not there:
                arr_a[o] = jnp.zeros_like(arr_a[o])
                arr_b[o] = jnp.zeros_like(arr_b[o])

        barrier = pltpu.get_barrier_semaphore()
        for other in neighbours:
            pl.semaphore_signal(barrier, inc=1, device_id={"dp": other}, device_id_type=MESH)
        pl.semaphore_wait(barrier, len(neighbours))

        def lag(o):
            return owned_lag(z) if o == z else LAG * (z if o > z else CHIPS - 1 - z)

        def own_copy(w, q, o):
            n = lax.rem(q, OWN)
            return pltpu.make_async_copy(piece(terms[w], w, 2 * o + core, q), slot(own_a, own_b, w, n, o), own_sem.at[o, w, n])

        def par_copy(w, q, o):
            n = lax.rem(q, PAR)
            return remote(piece(terms[w], w, 2 * o + 1 - core, q), slot(par_a, par_b, w, n, o), par_send.at[o, w, n], par_recv.at[o, w, n], partner)

        def sum_copy(w, q, o):
            n, k = lax.rem(q, SND), lax.rem(q, ARR)
            way = 1 if o > z else -1
            there = CHIPS if way < 0 and o == z - 1 else o
            return remote(slot(snd_a, snd_b, w, n, o), slot(arr_a, arr_b, w, k, there), snd_sem.at[o, w, n], arr_sem.at[there, w, k], me + 2 * way)

        def arr_wait(w, q, o):
            k = lax.rem(q, ARR)
            there = slot(arr_a, arr_b, w, k, o)
            remote(there, there, snd_sem.at[0, w, 0], arr_sem.at[o, w, k], me).wait_recv()

        def state_copies(w, q):
            n = lax.rem(q, MOM)
            return (
                pltpu.make_async_copy(piece(m_in[w], w, 0, q), slot(m_a, m_b, w, n), m_sem.at[w, n]),
                pltpu.make_async_copy(piece(v_in[w], w, 0, q), slot(v_a, v_b, w, n), v_sem.at[w, n]),
                pltpu.make_async_copy(piece(weights[w], w, me, q), slot(w_a, w_b, w, n), w_sem.at[w, n]),
            )

        def result_copies(w, q):
            n, k = lax.rem(q, NEW), lax.rem(q, GAT)
            there = piece(whole[w], w, me, q)
            local = [
                pltpu.make_async_copy(slot(mo_a, mo_b, w, n), piece(m_out[w], w, 0, q), mo_sem.at[w, n]),
                pltpu.make_async_copy(slot(vo_a, vo_b, w, n), piece(v_out[w], w, 0, q), vo_sem.at[w, n]),
            ]
            far = [remote(there, there, new_sem.at[0, w, n], gat_recv.at[z, w, k], me + 2)] if right else []
            far += [remote(there, there, new_sem.at[1, w, n], gat_recv.at[z, w, k], me - 2)] if left else []
            far += [remote(there, there, new_sem.at[2, w, n], pal_recv.at[w], partner)]
            return local, far

        def pass_copies(w, q, o):
            k = lax.rem(q, GAT)
            there = piece(whole[w], w, 2 * o + core, q)
            way = -1 if o > z else 1
            on = left if o > z else right
            far = [remote(there, there, gat_send.at[o, w, k], gat_recv.at[o, w, k], me + 2 * way)] if on else []
            return far + [remote(there, there, pal_send.at[o, w, k], pal_recv.at[w], partner)]

        def pass_wait(w, q, o):
            k = lax.rem(q, GAT)
            there = piece(whole[w], w, 2 * o + core, q)
            remote(there, there, gat_send.at[o, w, k], gat_recv.at[o, w, k], me).wait_recv()

        def at(i, k, lag):
            w = (k - lag) % 3
            return w, i + (k - lag - w) // 3

        def valid(q):
            return (q >= 0) & (q < PIECES)

        def fetch(i, k):
            for o in (*others, z):
                w, q = at(i, k, lag(o) - AHEAD)

                @pl.when(valid(q))
                def _(w=w, q=q, o=o):
                    @pl.when(q >= PAR)
                    def _():
                        par_copy(w, q - PAR, o).wait_send()

                    par_copy(w, q, o).start()
                    own_copy(w, q, o).start()
                    if o == z:
                        for copy in state_copies(w, q):
                            copy.start()

        def forward(i, k, o):
            w, q = at(i, k, lag(o))

            @pl.when(valid(q))
            def _():
                own_copy(w, q, o).wait()
                par_copy(w, q, o).wait_recv()
                if upstream(o):
                    arr_wait(w, q, o)

                @pl.when(q >= SND)
                def _():
                    sum_copy(w, q - SND, o).wait_send()

                own, par = slot(own_a, own_b, w, lax.rem(q, OWN), o), slot(par_a, par_b, w, lax.rem(q, PAR), o)
                arr, snd = slot(arr_a, arr_b, w, lax.rem(q, ARR), o), slot(snd_a, snd_b, w, lax.rem(q, SND), o)
                for r, c in chunks(w):
                    total = own[r, c].astype(jnp.float32) + par[r, c].astype(jnp.float32) + arr[r, c].astype(jnp.float32)
                    snd[r, c] = total.astype(jnp.bfloat16)
                sum_copy(w, q, o).start()

        def finish(i, k):
            w, q = at(i, k, lag(z))

            @pl.when(valid(q))
            def _():
                own_copy(w, q, z).wait()
                par_copy(w, q, z).wait_recv()
                for copy in state_copies(w, q):
                    copy.wait()
                if left:
                    arr_wait(w, q, z)
                if right:
                    arr_wait(w, q, CHIPS)

                @pl.when(q >= NEW)
                def _():
                    drain_result(w, q - NEW)

                own, par = slot(own_a, own_b, w, lax.rem(q, OWN), z), slot(par_a, par_b, w, lax.rem(q, PAR), z)
                one, two = slot(arr_a, arr_b, w, lax.rem(q, ARR), z), slot(arr_a, arr_b, w, lax.rem(q, ARR), CHIPS)
                n, k = lax.rem(q, MOM), lax.rem(q, NEW)
                m, v, old = slot(m_a, m_b, w, n), slot(v_a, v_b, w, n), slot(w_a, w_b, w, n)
                mo, vo, new = slot(mo_a, mo_b, w, k), slot(vo_a, vo_b, w, k), piece(whole[w], w, me, q)
                for r, c in chunks(w):
                    total = own[r, c].astype(jnp.float32) + par[r, c].astype(jnp.float32)
                    total = total + one[r, c].astype(jnp.float32) + two[r, c].astype(jnp.float32)
                    g = total.astype(jnp.bfloat16).astype(jnp.float32)
                    new[r, c], mo[r, c], vo[r, c] = adamw(old[r, c].astype(jnp.float32), m[r, c], v[r, c], g)
                local, far = result_copies(w, q)
                for copy in (*far, *local):
                    copy.start()

        def drain_result(w, q):
            local, far = result_copies(w, q)
            for copy in local:
                copy.wait()
            for copy in far:
                copy.wait_send()

        def pass_on(i, k, o):
            w, q = at(i, k, gather_lag(o, z))

            @pl.when(valid(q))
            def _():
                pass_wait(w, q, o)

                @pl.when(q >= GAT)
                def _():
                    for copy in pass_copies(w, q - GAT, o):
                        copy.wait_send()

                for copy in pass_copies(w, q, o):
                    copy.start()

        last = 3 * PIECES + max(gather_lag(o, z) for o in range(CHIPS))

        @pl.loop(-(AHEAD // 3), -(-last // 3))
        def _(i):
            for k in range(3):
                fetch(i, k)
                for o in others:
                    forward(i, k, o)
                finish(i, k)
                for o in others:
                    pass_on(i, k, o)

        def tail(ring, wait):
            @pl.loop(PIECES - ring, PIECES)
            def _(q):
                for w in range(3):
                    wait(w, q)

        def tail_par(w, q):
            for o in range(CHIPS):
                par_copy(w, q, o).wait_send()

        def tail_sum(w, q):
            for o in others:
                sum_copy(w, q, o).wait_send()

        def tail_pass(w, q):
            for o in others:
                for copy in pass_copies(w, q, o):
                    copy.wait_send()

        tail(PAR, tail_par)
        tail(SND, tail_sum)
        tail(NEW, drain_result)
        tail(GAT, tail_pass)
        for w in range(3):
            half = whole[w].at[0]
            pltpu.make_async_copy(half, half, pal_recv.at[w]).wait()

    for z in range(CHIPS):

        @pl.when(chip == z)
        def _(z=z):
            body(z)


def communicate(terms, weights, m, v):
    def ring(dtype, *lead):
        return [pltpu.VMEM((*lead[:-1], 2, lead[-1], *SHAPES[0]), dtype), pltpu.VMEM((*lead, *SHAPES[2]), dtype)]

    dma = pltpu.SemaphoreType.DMA
    bf16, f32 = jnp.bfloat16, jnp.float32
    return pl.pallas_call(
        kernel,
        out_shape=[pltpu.VMEM(a.shape, a.dtype) for a in weights] + [jax.ShapeDtypeStruct(a.shape, a.dtype) for a in (*m, *v)],
        in_specs=[pl.BlockSpec(memory_space=pl.ANY)] * 12,
        out_specs=[pl.BlockSpec(memory_space=pltpu.VMEM)] * 3 + [pl.BlockSpec(memory_space=pl.ANY)] * 6,
        scratch_shapes=[
            *ring(bf16, CHIPS, OWN),
            *ring(bf16, CHIPS, PAR),
            *ring(bf16, CHIPS + 1, ARR),
            *ring(bf16, CHIPS, SND),
            *ring(f32, MOM),
            *ring(f32, MOM),
            *ring(bf16, MOM),
            *ring(f32, NEW),
            *ring(f32, NEW),
            dma((CHIPS, 3, OWN)),
            dma((CHIPS, 3, PAR)),
            dma((CHIPS, 3, PAR)),
            dma((CHIPS + 1, 3, ARR)),
            dma((CHIPS, 3, SND)),
            dma((3, MOM)),
            dma((3, MOM)),
            dma((3, MOM)),
            dma((3, NEW)),
            dma((3, NEW)),
            dma((3, 3, NEW)),
            dma((CHIPS, 3, GAT)),
            dma((CHIPS, 3, GAT)),
            dma((CHIPS, 3, GAT)),
            dma((3,)),
        ],
        compiler_params=pltpu.CompilerParams(collective_id=0, has_side_effects=True, vmem_limit_bytes=LIMIT),
        name="sum_step_gather",
    )(*terms, *weights, *m, *v)


def hand_out(arrays):
    slots = (8, 4)

    def copy(*refs):
        held, moments, whole, out = refs[:3], refs[3:9], refs[9:12], refs[12:18]
        buffers, into, out_of, sent = refs[18:20], refs[20], refs[21], refs[22]
        down = [pltpu.make_async_copy(held[w].at[l], whole[w].at[l], sent.at[w, l]) for w in range(3) for l in range(2)]
        jobs, used = [], [0, 0]
        for l in range(2):
            for half in range(2):
                for n in range(6):
                    kind = n % 3 // 2
                    rows = pl.ds(half * (32, 512)[kind], (32, 512)[kind])
                    slot = used[kind] % slots[kind]
                    jobs.append((
                        (kind, slot),
                        pltpu.make_async_copy(moments[n].at[l, rows], buffers[kind].at[slot], into.at[kind, slot]),
                        pltpu.make_async_copy(buffers[kind].at[slot], out[n].at[l, rows], out_of.at[kind, slot]),
                    ))
                    used[kind] += 1
        ahead = sum(slots)
        for _, load, _ in jobs[:ahead]:
            load.start()
        for weight in down:
            weight.start()
        for n, (_, load, store) in enumerate(jobs):
            load.wait()
            store.start()
            if n >= 4 and n - 4 + ahead < len(jobs):
                jobs[n - 4][2].wait()
                jobs[n - 4 + ahead][1].start()
        for n, (_, _, store) in enumerate(jobs):
            if n + ahead >= len(jobs):
                store.wait()
        for weight in down:
            weight.wait()

    dma = pltpu.SemaphoreType.DMA
    return pl.pallas_call(
        copy,
        out_shape=[jax.ShapeDtypeStruct(a.shape, a.dtype) for a in arrays],
        in_specs=[pl.BlockSpec(memory_space=pl.ANY)] * 9,
        out_specs=[pl.BlockSpec(memory_space=pl.ANY)] * 9,
        scratch_shapes=[pltpu.VMEM((8, 32, 8192), jnp.float32), pltpu.VMEM((4, 512, 512), jnp.float32), dma((2, 8)), dma((2, 8)), dma((3, 2))],
        compiler_params=pltpu.CompilerParams(vmem_limit_bytes=LIMIT),
        name="hand_out",
    )(*[pltpu.with_memory_space_constraint(a, pltpu.VMEM if n < 3 else pltpu.HBM) for n, a in enumerate(arrays)])


def solution(mesh):
    def step(*arrays):
        terms, weights, m, v = (arrays[i : i + 3] for i in (0, 3, 6, 9))
        terms = [t.reshape(t.shape[1:]) for t in terms]
        return tuple(hand_out(communicate(terms, weights, m, v)))

    all_of, cut = P(None, None, None), P(None, "dp", None)
    return jax.shard_map(
        step,
        mesh=mesh,
        in_specs=(P(("rep", "dp"), None, None, None),) * 3 + (all_of,) * 3 + (cut,) * 6,
        out_specs=(P("rep", None, None),) * 3 + (P("rep", "dp", None),) * 6,
        check_vma=False,
    )
```

```python
import functools

import jax
import jax.numpy as jnp
from jax import lax
from jax.experimental import pallas as pl
from jax.experimental.pallas import tpu as pltpu
from jax.sharding import PartitionSpec as P

MESH = pl.DeviceIdType.MESH
CHIPS = 4
LAG = 2
LEAD = 2
AHEAD = 3
OWN, PAR, ARR, SND, MOM, NEW, GAT = 2, 3, 3, 2, 2, 2, 4
WEIGHTS = 3
PIECES = 64
SHAPES = ((16, 1024), (16, 1024), (32, 512))
KEPT = 2
GRANT = 6 << 20


def adamw(w, m, v, g):
    m = 0.9 * m + 0.1 * g
    v = 0.95 * v + 0.05 * g * g
    step = m * lax.rsqrt(v + 1e-8) + 0.1 * w
    return (w - 0.02 * step).astype(jnp.bfloat16), m, v


def piece(ref, w, block, q):
    layer, at = lax.div(q, 32), lax.rem(q, 32)
    if w < 2:
        row = pl.multiple_of(block * 64 + lax.div(at, 8) * 16, 16)
        return ref.at[layer, pl.ds(row, 16), pl.ds(pl.multiple_of(lax.rem(at, 8) * 1024, 1024), 1024)]
    return ref.at[layer, pl.ds(pl.multiple_of(block * 1024 + at * 32, 32), 32), :]


def chunks(w):
    rows, columns = SHAPES[w]
    for r in range(0, rows, 16):
        for c in range(0, columns, 512):
            yield pl.ds(r, 16), pl.ds(c, 512)


def late(owner):
    return 0 if owner in (0, CHIPS - 1) else LEAD


def owned_lag(z):
    return late(z) + LAG * max(z, CHIPS - 1 - z)


def gather_lag(owner, z):
    return owned_lag(owner) + LAG * abs(owner - z)


def kernel(*refs):
    refs = iter(refs)

    def take(n=WEIGHTS):
        return [next(refs) for _ in range(n)]

    terms, weights, m_in, v_in, whole, m_out, v_out = (take() for _ in range(7))
    own_ring, par_ring, arr_ring, snd_ring, m_ring, v_ring, w_ring = (take() for _ in range(7))
    mo_ring, vo_ring = take(KEPT), take(KEPT)
    own_sem, par_recv, par_send, arr_sem, snd_sem, m_sem, v_sem, w_sem, mo_sem, vo_sem, new_sem, gat_recv, gat_send, pal_send, pal_recv = refs

    me = lax.axis_index("dp")
    core = lax.rem(me, 2)
    chip = lax.div(me, 2)
    partner = me + 1 - 2 * core

    def remote(src, dst, send, recv, to):
        return pltpu.make_async_remote_copy(src_ref=src, dst_ref=dst, send_sem=send, recv_sem=recv, device_id={"dp": to}, device_id_type=MESH)

    def body(z):
        left, right = z > 0, z < CHIPS - 1
        others = sorted((o for o in range(CHIPS) if o != z), key=lambda o: -abs(o - z))
        neighbours = [partner] + ([me - 2] if left else []) + ([me + 2] if right else [])

        def upstream(o):
            return left if o > z else right

        barrier = pltpu.get_barrier_semaphore()
        for other in neighbours:
            pl.semaphore_signal(barrier, inc=1, device_id={"dp": other}, device_id_type=MESH)
        for o, there in (*((o, upstream(o)) for o in others), (z, left), (CHIPS, right)):
            if not there:
                for arr in arr_ring:
                    arr[o] = jnp.zeros_like(arr[o])

        pl.semaphore_wait(barrier, len(neighbours))

        def lag(o):
            return owned_lag(z) if o == z else late(o) + LAG * (z if o > z else CHIPS - 1 - z)

        def own_copy(w, q, o):
            n = lax.rem(q, OWN)
            return pltpu.make_async_copy(piece(terms[w], w, 2 * o + core, q), own_ring[w].at[o, n], own_sem.at[o, w, n])

        def par_copy(w, q, o):
            n = lax.rem(q, PAR)
            return remote(piece(terms[w], w, 2 * o + 1 - core, q), par_ring[w].at[o, n], par_send.at[o, w, n], par_recv.at[o, w, n], partner)

        def sum_copy(w, q, o):
            n, k = lax.rem(q, SND), lax.rem(q, ARR)
            way = 1 if o > z else -1
            there = CHIPS if way < 0 and o == z - 1 else o
            return remote(snd_ring[w].at[o, n], arr_ring[w].at[there, k], snd_sem.at[o, w, n], arr_sem.at[there, w, k], me + 2 * way)

        def arr_wait(w, q, o):
            k = lax.rem(q, ARR)
            there = arr_ring[w].at[o, k]
            remote(there, there, snd_sem.at[0, w, 0], arr_sem.at[o, w, k], me).wait_recv()

        def state_copies(w, q):
            n = lax.rem(q, MOM)
            return (
                pltpu.make_async_copy(piece(m_in[w], w, 0, q), m_ring[w].at[n], m_sem.at[w, n]),
                pltpu.make_async_copy(piece(v_in[w], w, 0, q), v_ring[w].at[n], v_sem.at[w, n]),
                pltpu.make_async_copy(piece(weights[w], w, me, q), w_ring[w].at[n], w_sem.at[w, n]),
            )

        def result_copies(w, q):
            n, k = lax.rem(q, NEW), lax.rem(q, GAT)
            new = there = piece(whole[w], w, me, q)
            local = []
            if w != KEPT:
                local.append(pltpu.make_async_copy(mo_ring[w].at[n], piece(m_out[w], w, 0, q), mo_sem.at[w, n]))
                local.append(pltpu.make_async_copy(vo_ring[w].at[n], piece(v_out[w], w, 0, q), vo_sem.at[w, n]))
            far = [remote(new, there, new_sem.at[0, w, n], gat_recv.at[z, w, k], me + 2)] if right else []
            far += [remote(new, there, new_sem.at[1, w, n], gat_recv.at[z, w, k], me - 2)] if left else []
            far += [remote(new, there, new_sem.at[2, w, n], pal_recv.at[w], partner)]
            return local, far

        def pass_copies(w, q, o):
            k = lax.rem(q, GAT)
            there = piece(whole[w], w, 2 * o + core, q)
            way = -1 if o > z else 1
            on = left if o > z else right
            far = [remote(there, there, gat_send.at[o, w, k], gat_recv.at[o, w, k], me + 2 * way)] if on else []
            return far + [remote(there, there, pal_send.at[o, w, k], pal_recv.at[w], partner)]

        def pass_wait(w, q, o):
            k = lax.rem(q, GAT)
            there = piece(whole[w], w, 2 * o + core, q)
            remote(there, there, gat_send.at[o, w, k], gat_recv.at[o, w, k], me).wait_recv()

        def at(i, k, lag):
            w = (k - lag) % WEIGHTS
            return w, i + (k - lag - w) // WEIGHTS

        def valid(q):
            return (q >= 0) & (q < PIECES)

        def fetch(i, k):
            for o in (*others, z):
                w, q = at(i, k, lag(o) - AHEAD)

                @pl.when(valid(q))
                def _(w=w, q=q, o=o):
                    @pl.when(q >= PAR)
                    def _():
                        par_copy(w, q - PAR, o).wait_send()

                    par_copy(w, q, o).start()
                    own_copy(w, q, o).start()
                    if o == z:
                        for copy in state_copies(w, q):
                            copy.start()

        def forward(i, k, o):
            w, q = at(i, k, lag(o))

            @pl.when(valid(q))
            def _():
                own_copy(w, q, o).wait()
                par_copy(w, q, o).wait_recv()
                if upstream(o):
                    arr_wait(w, q, o)

                @pl.when(q >= SND)
                def _():
                    sum_copy(w, q - SND, o).wait_send()

                own, par = own_ring[w].at[o, lax.rem(q, OWN)], par_ring[w].at[o, lax.rem(q, PAR)]
                arr, snd = arr_ring[w].at[o, lax.rem(q, ARR)], snd_ring[w].at[o, lax.rem(q, SND)]
                for r, c in chunks(w):
                    total = own[r, c].astype(jnp.float32) + par[r, c].astype(jnp.float32) + arr[r, c].astype(jnp.float32)
                    snd[r, c] = total.astype(jnp.bfloat16)
                sum_copy(w, q, o).start()

        def finish(i, k):
            w, q = at(i, k, lag(z))

            @pl.when(valid(q))
            def _():
                own_copy(w, q, z).wait()
                par_copy(w, q, z).wait_recv()
                for copy in state_copies(w, q):
                    copy.wait()
                if left:
                    arr_wait(w, q, z)
                if right:
                    arr_wait(w, q, CHIPS)

                @pl.when(q >= NEW)
                def _():
                    drain_result(w, q - NEW)

                own, par = own_ring[w].at[z, lax.rem(q, OWN)], par_ring[w].at[z, lax.rem(q, PAR)]
                one, two = arr_ring[w].at[z, lax.rem(q, ARR)], arr_ring[w].at[CHIPS, lax.rem(q, ARR)]
                n = lax.rem(q, MOM)
                m, v, old = m_ring[w].at[n], v_ring[w].at[n], w_ring[w].at[n]
                new, k = piece(whole[w], w, me, q), lax.rem(q, NEW)
                if w == KEPT:
                    mo, vo = piece(m_out[w], w, 0, q), piece(v_out[w], w, 0, q)
                else:
                    mo, vo = mo_ring[w].at[k], vo_ring[w].at[k]
                for r, c in chunks(w):
                    total = own[r, c].astype(jnp.float32) + par[r, c].astype(jnp.float32)
                    total = total + one[r, c].astype(jnp.float32) + two[r, c].astype(jnp.float32)
                    g = total.astype(jnp.bfloat16).astype(jnp.float32)
                    new[r, c], mo[r, c], vo[r, c] = adamw(old[r, c].astype(jnp.float32), m[r, c], v[r, c], g)
                local, far = result_copies(w, q)
                for copy in (*far, *local):
                    copy.start()

        def drain_result(w, q):
            local, far = result_copies(w, q)
            for copy in local:
                copy.wait()
            for copy in far:
                copy.wait_send()

        def pass_on(i, k, o):
            w, q = at(i, k, gather_lag(o, z))

            @pl.when(valid(q))
            def _():
                pass_wait(w, q, o)

                @pl.when(q >= GAT)
                def _():
                    for copy in pass_copies(w, q - GAT, o):
                        copy.wait_send()

                for copy in pass_copies(w, q, o):
                    copy.start()

        last = WEIGHTS * PIECES + max(gather_lag(o, z) for o in range(CHIPS))

        @pl.loop(-((AHEAD + WEIGHTS - 1) // WEIGHTS), -(-last // WEIGHTS))
        def _(i):
            for k in range(WEIGHTS):
                fetch(i, k)
                for o in others:
                    forward(i, k, o)
                finish(i, k)
                for o in others:
                    pass_on(i, k, o)

        def tail(ring, wait):
            @pl.loop(PIECES - ring, PIECES)
            def _(q):
                for w in range(WEIGHTS):
                    wait(w, q)

        def tail_par(w, q):
            for o in range(CHIPS):
                par_copy(w, q, o).wait_send()

        def tail_sum(w, q):
            for o in others:
                sum_copy(w, q, o).wait_send()

        def tail_pass(w, q):
            for o in others:
                for copy in pass_copies(w, q, o):
                    copy.wait_send()

        tail(PAR, tail_par)
        tail(SND, tail_sum)
        tail(NEW, drain_result)
        tail(GAT, tail_pass)
        for w in range(WEIGHTS):
            half = whole[w].at[0]
            pltpu.make_async_copy(half, half, pal_recv.at[w]).wait()

    for z in range(CHIPS):

        @pl.when(chip == z)
        def _(z=z):
            body(z)


def communicate(terms, weights, m, v):
    def ring(dtype, *lead, of=WEIGHTS):
        return [pltpu.VMEM((*lead, *SHAPES[w]), dtype) for w in range(of)]

    def moments(arrays):
        return [(pltpu.VMEM if w == KEPT else jax.ShapeDtypeStruct)(a.shape, a.dtype) for w, a in enumerate(arrays)]

    dma = pltpu.SemaphoreType.DMA
    bf16, f32 = jnp.bfloat16, jnp.float32
    spaces = [pltpu.VMEM if w == KEPT else pl.ANY for w in range(WEIGHTS)]
    return pl.pallas_call(
        kernel,
        out_shape=[pltpu.VMEM(a.shape, a.dtype) for a in weights] + moments(m) + moments(v),
        in_specs=[pl.BlockSpec(memory_space=pl.ANY)] * (4 * WEIGHTS),
        out_specs=[pl.BlockSpec(memory_space=space) for space in (*[pltpu.VMEM] * WEIGHTS, *spaces, *spaces)],
        scratch_shapes=[
            *ring(bf16, CHIPS, OWN),
            *ring(bf16, CHIPS, PAR),
            *ring(bf16, CHIPS + 1, ARR),
            *ring(bf16, CHIPS, SND),
            *ring(f32, MOM),
            *ring(f32, MOM),
            *ring(bf16, MOM),
            *ring(f32, NEW, of=KEPT),
            *ring(f32, NEW, of=KEPT),
            dma((CHIPS, WEIGHTS, OWN)),
            dma((CHIPS, WEIGHTS, PAR)),
            dma((CHIPS, WEIGHTS, PAR)),
            dma((CHIPS + 1, WEIGHTS, ARR)),
            dma((CHIPS, WEIGHTS, SND)),
            dma((WEIGHTS, MOM)),
            dma((WEIGHTS, MOM)),
            dma((WEIGHTS, MOM)),
            dma((WEIGHTS, NEW)),
            dma((WEIGHTS, NEW)),
            dma((3, WEIGHTS, NEW)),
            dma((CHIPS, WEIGHTS, GAT)),
            dma((CHIPS, WEIGHTS, GAT)),
            dma((CHIPS, WEIGHTS, GAT)),
            dma((WEIGHTS,)),
        ],
        compiler_params=pltpu.CompilerParams(collective_id=0, has_side_effects=True, vmem_limit_bytes=GRANT),
        name="sum_step_gather",
    )(*terms, *weights, *m, *v)


def hand_out(arrays):
    kept = (0, 1, 2, 3 + KEPT, 6 + KEPT)
    rest = [n for n in range(9) if n not in kept]
    slots = 5

    def copy(*refs):
        given, out, buffer, into, out_of, sent = refs[:9], refs[9:18], *refs[18:]
        down = [pltpu.make_async_copy(given[n].at[l], out[n].at[l], sent.at[n, l]) for n in kept for l in range(2)]
        parts = [(n, l, pl.ds(half * 32, 32)) for n in rest for l in range(2) for half in range(2)]
        loads, stores = [], []
        for j, (n, l, rows) in enumerate(parts):
            slot = j % slots
            loads.append(pltpu.make_async_copy(given[n].at[l, rows], buffer.at[slot], into.at[slot]))
            stores.append(pltpu.make_async_copy(buffer.at[slot], out[n].at[l, rows], out_of.at[slot]))
        for load in loads[:slots]:
            load.start()
        for done in down:
            done.start()
        for j in range(len(parts)):
            loads[j].wait()
            stores[j].start()
            if j >= 2 and j - 2 + slots < len(parts):
                stores[j - 2].wait()
                loads[j - 2 + slots].start()
        for store in stores[-slots:]:
            store.wait()
        for done in down:
            done.wait()

    dma = pltpu.SemaphoreType.DMA
    return pl.pallas_call(
        copy,
        out_shape=[jax.ShapeDtypeStruct(a.shape, a.dtype) for a in arrays],
        in_specs=[pl.BlockSpec(memory_space=pl.ANY)] * 9,
        out_specs=[pl.BlockSpec(memory_space=pl.ANY)] * 9,
        scratch_shapes=[pltpu.VMEM((slots, 32, 8192), jnp.float32), dma((slots,)), dma((slots,)), dma((9, 2))],
        compiler_params=pltpu.CompilerParams(vmem_limit_bytes=GRANT),
        name="hand_out",
    )(*[pltpu.with_memory_space_constraint(a, pltpu.VMEM if n in kept else pltpu.HBM) for n, a in enumerate(arrays)])


def solution(mesh):
    def step(*arrays):
        terms, weights, m, v = (arrays[i : i + 3] for i in (0, 3, 6, 9))
        terms = [t.reshape(t.shape[1:]) for t in terms]
        return tuple(hand_out(communicate(terms, weights, m, v)))

    all_of, cut = P(None, None, None), P(None, "dp", None)
    return jax.shard_map(
        step,
        mesh=mesh,
        in_specs=(P(("rep", "dp"), None, None, None),) * 3 + (all_of,) * 3 + (cut,) * 6,
        out_specs=(P("rep", None, None),) * 3 + (P("rep", "dp", None),) * 6,
        check_vma=False,
    )
```

```python
import functools

import jax
import jax.numpy as jnp
from jax import lax
from jax.experimental import pallas as pl
from jax.experimental.pallas import tpu as pltpu
from jax.sharding import PartitionSpec as P

MESH = pl.DeviceIdType.MESH
CHIPS = 4
LAG = 2
LEAD = 2
AHEAD = 3
OWN, PAR, ARR, SND, MOM, NEW, GAT = 2, 3, 3, 2, 2, 2, 4
WEIGHTS = 3
PIECES = 64
SHAPES = ((16, 1024), (16, 1024), (32, 512))
KEPT = 2
GRANT = 6 << 20


def adamw(w, m, v, g):
    m = 0.9 * m + 0.1 * g
    v = 0.95 * v + 0.05 * g * g
    step = m * lax.rsqrt(v + 1e-8) + 0.1 * w
    return (w - 0.02 * step).astype(jnp.bfloat16), m, v


def piece(ref, w, block, q):
    layer, at = lax.div(q, 32), lax.rem(q, 32)
    if w < 2:
        row = pl.multiple_of(block * 64 + lax.div(at, 8) * 16, 16)
        return ref.at[layer, pl.ds(row, 16), pl.ds(pl.multiple_of(lax.rem(at, 8) * 1024, 1024), 1024)]
    return ref.at[layer, pl.ds(pl.multiple_of(block * 1024 + at * 32, 32), 32), :]


def chunks(w):
    rows, columns = SHAPES[w]
    for r in range(0, rows, 16):
        for c in range(0, columns, 512):
            yield pl.ds(r, 16), pl.ds(c, 512)


def late(owner):
    return 0 if owner in (0, CHIPS - 1) else LEAD


def owned_lag(z):
    return late(z) + LAG * max(z, CHIPS - 1 - z)


def gather_lag(owner, z):
    return owned_lag(owner) + LAG * abs(owner - z)


def kernel(*refs):
    refs = iter(refs)

    def take(n=WEIGHTS):
        return [next(refs) for _ in range(n)]

    terms, weights, m_in, v_in, whole, m_out, v_out = (take() for _ in range(7))
    own_ring, par_ring, arr_ring, snd_ring, m_ring, v_ring, w_ring = (take() for _ in range(7))
    mo_ring, vo_ring = take(KEPT), take(KEPT)
    own_sem, par_recv, par_send, arr_sem, snd_sem, m_sem, v_sem, w_sem, mo_sem, vo_sem, new_sem, gat_recv, gat_send, pal_send, pal_recv = refs

    me = lax.axis_index("dp")
    core = lax.rem(me, 2)
    chip = lax.div(me, 2)
    partner = me + 1 - 2 * core

    def remote(src, dst, send, recv, to):
        return pltpu.make_async_remote_copy(src_ref=src, dst_ref=dst, send_sem=send, recv_sem=recv, device_id={"dp": to}, device_id_type=MESH)

    def body(z):
        left, right = z > 0, z < CHIPS - 1
        others = sorted((o for o in range(CHIPS) if o != z), key=lambda o: -abs(o - z))
        neighbours = [partner] + ([me - 2] if left else []) + ([me + 2] if right else [])

        def upstream(o):
            return left if o > z else right

        barrier = pltpu.get_barrier_semaphore()
        for other in neighbours:
            pl.semaphore_signal(barrier, inc=1, device_id={"dp": other}, device_id_type=MESH)
        for o, there in (*((o, upstream(o)) for o in others), (z, left), (CHIPS, right)):
            if not there:
                for arr in arr_ring:
                    arr[o] = jnp.zeros_like(arr[o])

        pl.semaphore_wait(barrier, len(neighbours))

        def lag(o):
            return owned_lag(z) if o == z else late(o) + LAG * (z if o > z else CHIPS - 1 - z)

        def own_copy(w, q, o):
            n = lax.rem(q, OWN)
            return pltpu.make_async_copy(piece(terms[w], w, 2 * o + core, q), own_ring[w].at[o, n], own_sem.at[o, w, n])

        def par_copy(w, q, o):
            n = lax.rem(q, PAR)
            return remote(piece(terms[w], w, 2 * o + 1 - core, q), par_ring[w].at[o, n], par_send.at[o, w, n], par_recv.at[o, w, n], partner)

        def sum_copy(w, q, o):
            n, k = lax.rem(q, SND), lax.rem(q, ARR)
            way = 1 if o > z else -1
            there = CHIPS if way < 0 and o == z - 1 else o
            return remote(snd_ring[w].at[o, n], arr_ring[w].at[there, k], snd_sem.at[o, w, n], arr_sem.at[there, w, k], me + 2 * way)

        def arr_wait(w, q, o):
            k = lax.rem(q, ARR)
            there = arr_ring[w].at[o, k]
            remote(there, there, snd_sem.at[0, w, 0], arr_sem.at[o, w, k], me).wait_recv()

        def state_copies(w, q):
            n = lax.rem(q, MOM)
            return (
                pltpu.make_async_copy(piece(m_in[w], w, 0, q), m_ring[w].at[n], m_sem.at[w, n]),
                pltpu.make_async_copy(piece(v_in[w], w, 0, q), v_ring[w].at[n], v_sem.at[w, n]),
                pltpu.make_async_copy(piece(weights[w], w, me, q), w_ring[w].at[n], w_sem.at[w, n]),
            )

        def result_copies(w, q):
            n, k = lax.rem(q, NEW), lax.rem(q, GAT)
            new = there = piece(whole[w], w, me, q)
            local = []
            if w != KEPT:
                local.append(pltpu.make_async_copy(mo_ring[w].at[n], piece(m_out[w], w, 0, q), mo_sem.at[w, n]))
                local.append(pltpu.make_async_copy(vo_ring[w].at[n], piece(v_out[w], w, 0, q), vo_sem.at[w, n]))
            far = [remote(new, there, new_sem.at[0, w, n], gat_recv.at[z, w, k], me + 2)] if right else []
            far += [remote(new, there, new_sem.at[1, w, n], gat_recv.at[z, w, k], me - 2)] if left else []
            far += [remote(new, there, new_sem.at[2, w, n], pal_recv.at[w], partner)]
            return local, far

        def pass_copies(w, q, o):
            k = lax.rem(q, GAT)
            there = piece(whole[w], w, 2 * o + core, q)
            way = -1 if o > z else 1
            on = left if o > z else right
            far = [remote(there, there, gat_send.at[o, w, k], gat_recv.at[o, w, k], me + 2 * way)] if on else []
            return far + [remote(there, there, pal_send.at[o, w, k], pal_recv.at[w], partner)]

        def pass_wait(w, q, o):
            k = lax.rem(q, GAT)
            there = piece(whole[w], w, 2 * o + core, q)
            remote(there, there, gat_send.at[o, w, k], gat_recv.at[o, w, k], me).wait_recv()

        def at(i, k, lag):
            w = (k - lag) % WEIGHTS
            return w, i + (k - lag - w) // WEIGHTS

        def valid(q):
            return (q >= 0) & (q < PIECES)

        def fetch(i, k):
            for o in (*others, z):
                w, q = at(i, k, lag(o) - AHEAD)

                @pl.when(valid(q))
                def _(w=w, q=q, o=o):
                    @pl.when(q >= PAR)
                    def _():
                        par_copy(w, q - PAR, o).wait_send()

                    par_copy(w, q, o).start()
                    own_copy(w, q, o).start()
                    if o == z:
                        for copy in state_copies(w, q):
                            copy.start()

        def forward(i, k, o):
            w, q = at(i, k, lag(o))

            @pl.when(valid(q))
            def _():
                own_copy(w, q, o).wait()
                par_copy(w, q, o).wait_recv()
                if upstream(o):
                    arr_wait(w, q, o)

                @pl.when(q >= SND)
                def _():
                    sum_copy(w, q - SND, o).wait_send()

                own, par = own_ring[w].at[o, lax.rem(q, OWN)], par_ring[w].at[o, lax.rem(q, PAR)]
                arr, snd = arr_ring[w].at[o, lax.rem(q, ARR)], snd_ring[w].at[o, lax.rem(q, SND)]
                for r, c in chunks(w):
                    total = own[r, c].astype(jnp.float32) + par[r, c].astype(jnp.float32) + arr[r, c].astype(jnp.float32)
                    snd[r, c] = total.astype(jnp.bfloat16)
                sum_copy(w, q, o).start()

        def finish(i, k):
            w, q = at(i, k, lag(z))

            @pl.when(valid(q))
            def _():
                own_copy(w, q, z).wait()
                par_copy(w, q, z).wait_recv()
                for copy in state_copies(w, q):
                    copy.wait()
                if left:
                    arr_wait(w, q, z)
                if right:
                    arr_wait(w, q, CHIPS)

                @pl.when(q >= NEW)
                def _():
                    drain_result(w, q - NEW)

                own, par = own_ring[w].at[z, lax.rem(q, OWN)], par_ring[w].at[z, lax.rem(q, PAR)]
                one, two = arr_ring[w].at[z, lax.rem(q, ARR)], arr_ring[w].at[CHIPS, lax.rem(q, ARR)]
                n = lax.rem(q, MOM)
                m, v, old = m_ring[w].at[n], v_ring[w].at[n], w_ring[w].at[n]
                new, k = piece(whole[w], w, me, q), lax.rem(q, NEW)
                if w == KEPT:
                    mo, vo = piece(m_out[w], w, 0, q), piece(v_out[w], w, 0, q)
                else:
                    mo, vo = mo_ring[w].at[k], vo_ring[w].at[k]
                for r, c in chunks(w):
                    total = own[r, c].astype(jnp.float32) + par[r, c].astype(jnp.float32)
                    total = total + one[r, c].astype(jnp.float32) + two[r, c].astype(jnp.float32)
                    g = total.astype(jnp.bfloat16).astype(jnp.float32)
                    new[r, c], mo[r, c], vo[r, c] = adamw(old[r, c].astype(jnp.float32), m[r, c], v[r, c], g)
                local, far = result_copies(w, q)
                for copy in (*far, *local):
                    copy.start()

        def drain_result(w, q):
            local, far = result_copies(w, q)
            for copy in local:
                copy.wait()
            for copy in far:
                copy.wait_send()

        def pass_on(i, k, o):
            w, q = at(i, k, gather_lag(o, z))

            @pl.when(valid(q))
            def _():
                pass_wait(w, q, o)

                @pl.when(q >= GAT)
                def _():
                    for copy in pass_copies(w, q - GAT, o):
                        copy.wait_send()

                for copy in pass_copies(w, q, o):
                    copy.start()

        last = WEIGHTS * PIECES + max(gather_lag(o, z) for o in range(CHIPS))

        @pl.loop(-((AHEAD + WEIGHTS - 1) // WEIGHTS), -(-last // WEIGHTS))
        def _(i):
            for k in range(WEIGHTS):
                fetch(i, k)
                for o in others:
                    forward(i, k, o)
                finish(i, k)
                for o in others:
                    pass_on(i, k, o)

        def tail(ring, wait):
            @pl.loop(PIECES - ring, PIECES)
            def _(q):
                for w in range(WEIGHTS):
                    wait(w, q)

        def tail_par(w, q):
            for o in range(CHIPS):
                par_copy(w, q, o).wait_send()

        def tail_sum(w, q):
            for o in others:
                sum_copy(w, q, o).wait_send()

        def tail_pass(w, q):
            for o in others:
                for copy in pass_copies(w, q, o):
                    copy.wait_send()

        tail(PAR, tail_par)
        tail(SND, tail_sum)
        tail(NEW, drain_result)
        tail(GAT, tail_pass)
        for w in range(WEIGHTS):
            half = whole[w].at[0]
            pltpu.make_async_copy(half, half, pal_recv.at[w]).wait()

    for z in range(CHIPS):

        @pl.when(chip == z)
        def _(z=z):
            body(z)


def communicate(terms, weights, m, v):
    def ring(dtype, *lead, of=WEIGHTS):
        return [pltpu.VMEM((*lead, *SHAPES[w]), dtype) for w in range(of)]

    def moments(arrays):
        return [(pltpu.VMEM if w == KEPT else jax.ShapeDtypeStruct)(a.shape, a.dtype) for w, a in enumerate(arrays)]

    dma = pltpu.SemaphoreType.DMA
    bf16, f32 = jnp.bfloat16, jnp.float32
    spaces = [pltpu.VMEM if w == KEPT else pl.ANY for w in range(WEIGHTS)]
    return pl.pallas_call(
        kernel,
        out_shape=[pltpu.VMEM(a.shape, a.dtype) for a in weights] + moments(m) + moments(v),
        in_specs=[pl.BlockSpec(memory_space=pl.ANY)] * (4 * WEIGHTS),
        out_specs=[pl.BlockSpec(memory_space=space) for space in (*[pltpu.VMEM] * WEIGHTS, *spaces, *spaces)],
        scratch_shapes=[
            *ring(bf16, CHIPS, OWN),
            *ring(bf16, CHIPS, PAR),
            *ring(bf16, CHIPS + 1, ARR),
            *ring(bf16, CHIPS, SND),
            *ring(f32, MOM),
            *ring(f32, MOM),
            *ring(bf16, MOM),
            *ring(f32, NEW, of=KEPT),
            *ring(f32, NEW, of=KEPT),
            dma((CHIPS, WEIGHTS, OWN)),
            dma((CHIPS, WEIGHTS, PAR)),
            dma((CHIPS, WEIGHTS, PAR)),
            dma((CHIPS + 1, WEIGHTS, ARR)),
            dma((CHIPS, WEIGHTS, SND)),
            dma((WEIGHTS, MOM)),
            dma((WEIGHTS, MOM)),
            dma((WEIGHTS, MOM)),
            dma((WEIGHTS, NEW)),
            dma((WEIGHTS, NEW)),
            dma((3, WEIGHTS, NEW)),
            dma((CHIPS, WEIGHTS, GAT)),
            dma((CHIPS, WEIGHTS, GAT)),
            dma((CHIPS, WEIGHTS, GAT)),
            dma((WEIGHTS,)),
        ],
        compiler_params=pltpu.CompilerParams(collective_id=0, has_side_effects=True, vmem_limit_bytes=GRANT),
        name="sum_step_gather",
    )(*terms, *weights, *m, *v)


def hand_out(arrays):
    kept = (0, 1, 2, 3 + KEPT, 6 + KEPT)
    rest = [n for n in range(9) if n not in kept]
    slots = 5

    def copy(*refs):
        given, out, buffer, into, out_of, sent = refs[:9], refs[9:18], *refs[18:]
        down = []
        for part in range(8):
            for n in kept:
                rows = out[n].shape[1] // 4
                where = part // 4, pl.ds(part % 4 * rows, rows)
                down.append(pltpu.make_async_copy(given[n].at[where], out[n].at[where], sent.at[n, part]))
        parts = [(n, l, pl.ds(half * 32, 32)) for n in rest for l in range(2) for half in range(2)]
        loads, stores = [], []
        for j, (n, l, rows) in enumerate(parts):
            slot = j % slots
            loads.append(pltpu.make_async_copy(given[n].at[l, rows], buffer.at[slot], into.at[slot]))
            stores.append(pltpu.make_async_copy(buffer.at[slot], out[n].at[l, rows], out_of.at[slot]))
        for load in loads[:slots]:
            load.start()
        for done in down[:8]:
            done.start()
        for j in range(len(parts)):
            loads[j].wait()
            stores[j].start()
            for done in down[8 + 2 * j : 10 + 2 * j]:
                done.start()
            if j >= 2 and j - 2 + slots < len(parts):
                stores[j - 2].wait()
                loads[j - 2 + slots].start()
        for store in stores[-slots:]:
            store.wait()
        for done in down:
            done.wait()

    dma = pltpu.SemaphoreType.DMA
    return pl.pallas_call(
        copy,
        out_shape=[jax.ShapeDtypeStruct(a.shape, a.dtype) for a in arrays],
        in_specs=[pl.BlockSpec(memory_space=pl.ANY)] * 9,
        out_specs=[pl.BlockSpec(memory_space=pl.ANY)] * 9,
        scratch_shapes=[pltpu.VMEM((slots, 32, 8192), jnp.float32), dma((slots,)), dma((slots,)), dma((9, 8))],
        compiler_params=pltpu.CompilerParams(vmem_limit_bytes=GRANT),
        name="hand_out",
    )(*[pltpu.with_memory_space_constraint(a, pltpu.VMEM if n in kept else pltpu.HBM) for n, a in enumerate(arrays)])


def solution(mesh):
    def step(*arrays):
        terms, weights, m, v = (arrays[i : i + 3] for i in (0, 3, 6, 9))
        terms = [t.reshape(t.shape[1:]) for t in terms]
        return tuple(hand_out(communicate(terms, weights, m, v)))

    all_of, cut = P(None, None, None), P(None, "dp", None)
    return jax.shard_map(
        step,
        mesh=mesh,
        in_specs=(P(("rep", "dp"), None, None, None),) * 3 + (all_of,) * 3 + (cut,) * 6,
        out_specs=(P("rep", None, None),) * 3 + (P("rep", "dp", None),) * 6,
        check_vma=False,
    )
```

```python
import functools

import jax
import jax.numpy as jnp
from jax import lax
from jax.experimental import pallas as pl
from jax.experimental.pallas import tpu as pltpu
from jax.sharding import PartitionSpec as P

MESH = pl.DeviceIdType.MESH
CHIPS = 4
LAG = 2
LEAD = 4
AHEAD = 3
OWN, PAR, ARR, SND, MOM, NEW, GAT = 2, 3, 3, 2, 2, 2, 4
WEIGHTS = 3
PIECES = 64
SHAPES = ((16, 1024), (16, 1024), (32, 512))
KEPT = 2
GRANT = 6 << 20


def adamw(w, m, v, g):
    m = 0.9 * m + 0.1 * g
    v = 0.95 * v + 0.05 * g * g
    step = m * lax.rsqrt(v + 1e-8) + 0.1 * w
    return (w - 0.02 * step).astype(jnp.bfloat16), m, v


def piece(ref, w, block, q):
    layer, at = lax.div(q, 32), lax.rem(q, 32)
    if w < 2:
        row = pl.multiple_of(block * 64 + lax.div(at, 8) * 16, 16)
        return ref.at[layer, pl.ds(row, 16), pl.ds(pl.multiple_of(lax.rem(at, 8) * 1024, 1024), 1024)]
    return ref.at[layer, pl.ds(pl.multiple_of(block * 1024 + at * 32, 32), 32), :]


def chunks(w):
    rows, columns = SHAPES[w]
    for r in range(0, rows, 16):
        for c in range(0, columns, 512):
            yield pl.ds(r, 16), pl.ds(c, 512)


def late(owner):
    return 0 if owner in (0, CHIPS - 1) else LEAD


def owned_lag(z):
    return late(z) + LAG * max(z, CHIPS - 1 - z)


def gather_lag(owner, z):
    return owned_lag(owner) + LAG * abs(owner - z)


def kernel(*refs):
    refs = iter(refs)

    def take(n=WEIGHTS):
        return [next(refs) for _ in range(n)]

    terms, weights, m_in, v_in, whole, m_out, v_out = (take() for _ in range(7))
    own_ring, par_ring, arr_ring, snd_ring, m_ring, v_ring, w_ring = (take() for _ in range(7))
    mo_ring, vo_ring = take(KEPT), take(KEPT)
    own_sem, par_recv, par_send, arr_sem, snd_sem, m_sem, v_sem, w_sem, mo_sem, vo_sem, new_sem, gat_recv, gat_send, pal_send, pal_recv = refs

    me = lax.axis_index("dp")
    core = lax.rem(me, 2)
    chip = lax.div(me, 2)
    partner = me + 1 - 2 * core

    def remote(src, dst, send, recv, to):
        return pltpu.make_async_remote_copy(src_ref=src, dst_ref=dst, send_sem=send, recv_sem=recv, device_id={"dp": to}, device_id_type=MESH)

    def body(z):
        left, right = z > 0, z < CHIPS - 1
        others = sorted((o for o in range(CHIPS) if o != z), key=lambda o: -abs(o - z))
        neighbours = [partner] + ([me - 2] if left else []) + ([me + 2] if right else [])

        def upstream(o):
            return left if o > z else right

        barrier = pltpu.get_barrier_semaphore()
        for other in neighbours:
            pl.semaphore_signal(barrier, inc=1, device_id={"dp": other}, device_id_type=MESH)
        for o, there in (*((o, upstream(o)) for o in others), (z, left), (CHIPS, right)):
            if not there:
                for arr in arr_ring:
                    arr[o] = jnp.zeros_like(arr[o])

        pl.semaphore_wait(barrier, len(neighbours))

        def lag(o):
            return owned_lag(z) if o == z else late(o) + LAG * (z if o > z else CHIPS - 1 - z)

        def own_copy(w, q, o):
            n = lax.rem(q, OWN)
            return pltpu.make_async_copy(piece(terms[w], w, 2 * o + core, q), own_ring[w].at[o, n], own_sem.at[o, w, n])

        def par_copy(w, q, o):
            n = lax.rem(q, PAR)
            return remote(piece(terms[w], w, 2 * o + 1 - core, q), par_ring[w].at[o, n], par_send.at[o, w, n], par_recv.at[o, w, n], partner)

        def sum_copy(w, q, o):
            n, k = lax.rem(q, SND), lax.rem(q, ARR)
            way = 1 if o > z else -1
            there = CHIPS if way < 0 and o == z - 1 else o
            return remote(snd_ring[w].at[o, n], arr_ring[w].at[there, k], snd_sem.at[o, w, n], arr_sem.at[there, w, k], me + 2 * way)

        def arr_wait(w, q, o):
            k = lax.rem(q, ARR)
            there = arr_ring[w].at[o, k]
            remote(there, there, snd_sem.at[0, w, 0], arr_sem.at[o, w, k], me).wait_recv()

        def state_copies(w, q):
            n = lax.rem(q, MOM)
            return (
                pltpu.make_async_copy(piece(m_in[w], w, 0, q), m_ring[w].at[n], m_sem.at[w, n]),
                pltpu.make_async_copy(piece(v_in[w], w, 0, q), v_ring[w].at[n], v_sem.at[w, n]),
                pltpu.make_async_copy(piece(weights[w], w, me, q), w_ring[w].at[n], w_sem.at[w, n]),
            )

        def result_copies(w, q):
            n, k = lax.rem(q, NEW), lax.rem(q, GAT)
            new = there = piece(whole[w], w, me, q)
            local = []
            if w != KEPT:
                local.append(pltpu.make_async_copy(mo_ring[w].at[n], piece(m_out[w], w, 0, q), mo_sem.at[w, n]))
                local.append(pltpu.make_async_copy(vo_ring[w].at[n], piece(v_out[w], w, 0, q), vo_sem.at[w, n]))
            far = [remote(new, there, new_sem.at[0, w, n], gat_recv.at[z, w, k], me + 2)] if right else []
            far += [remote(new, there, new_sem.at[1, w, n], gat_recv.at[z, w, k], me - 2)] if left else []
            far += [remote(new, there, new_sem.at[2, w, n], pal_recv.at[w], partner)]
            return local, far

        def pass_copies(w, q, o):
            k = lax.rem(q, GAT)
            there = piece(whole[w], w, 2 * o + core, q)
            way = -1 if o > z else 1
            on = left if o > z else right
            far = [remote(there, there, gat_send.at[o, w, k], gat_recv.at[o, w, k], me + 2 * way)] if on else []
            return far + [remote(there, there, pal_send.at[o, w, k], pal_recv.at[w], partner)]

        def pass_wait(w, q, o):
            k = lax.rem(q, GAT)
            there = piece(whole[w], w, 2 * o + core, q)
            remote(there, there, gat_send.at[o, w, k], gat_recv.at[o, w, k], me).wait_recv()

        def at(i, k, lag):
            w = (k - lag) % WEIGHTS
            return w, i + (k - lag - w) // WEIGHTS

        def valid(q):
            return (q >= 0) & (q < PIECES)

        def fetch(i, k):
            for o in (*others, z):
                w, q = at(i, k, lag(o) - AHEAD)

                @pl.when(valid(q))
                def _(w=w, q=q, o=o):
                    @pl.when(q >= PAR)
                    def _():
                        par_copy(w, q - PAR, o).wait_send()

                    par_copy(w, q, o).start()
                    own_copy(w, q, o).start()
                    if o == z:
                        for copy in state_copies(w, q):
                            copy.start()

        def forward(i, k, o):
            w, q = at(i, k, lag(o))

            @pl.when(valid(q))
            def _():
                own_copy(w, q, o).wait()
                par_copy(w, q, o).wait_recv()
                if upstream(o):
                    arr_wait(w, q, o)

                @pl.when(q >= SND)
                def _():
                    sum_copy(w, q - SND, o).wait_send()

                own, par = own_ring[w].at[o, lax.rem(q, OWN)], par_ring[w].at[o, lax.rem(q, PAR)]
                arr, snd = arr_ring[w].at[o, lax.rem(q, ARR)], snd_ring[w].at[o, lax.rem(q, SND)]
                for r, c in chunks(w):
                    total = own[r, c].astype(jnp.float32) + par[r, c].astype(jnp.float32) + arr[r, c].astype(jnp.float32)
                    snd[r, c] = total.astype(jnp.bfloat16)
                sum_copy(w, q, o).start()

        def finish(i, k):
            w, q = at(i, k, lag(z))

            @pl.when(valid(q))
            def _():
                own_copy(w, q, z).wait()
                par_copy(w, q, z).wait_recv()
                for copy in state_copies(w, q):
                    copy.wait()
                if left:
                    arr_wait(w, q, z)
                if right:
                    arr_wait(w, q, CHIPS)

                @pl.when(q >= NEW)
                def _():
                    drain_result(w, q - NEW)

                own, par = own_ring[w].at[z, lax.rem(q, OWN)], par_ring[w].at[z, lax.rem(q, PAR)]
                one, two = arr_ring[w].at[z, lax.rem(q, ARR)], arr_ring[w].at[CHIPS, lax.rem(q, ARR)]
                n = lax.rem(q, MOM)
                m, v, old = m_ring[w].at[n], v_ring[w].at[n], w_ring[w].at[n]
                new, k = piece(whole[w], w, me, q), lax.rem(q, NEW)
                if w == KEPT:
                    mo, vo = piece(m_out[w], w, 0, q), piece(v_out[w], w, 0, q)
                else:
                    mo, vo = mo_ring[w].at[k], vo_ring[w].at[k]
                for r, c in chunks(w):
                    total = own[r, c].astype(jnp.float32) + par[r, c].astype(jnp.float32)
                    total = total + one[r, c].astype(jnp.float32) + two[r, c].astype(jnp.float32)
                    g = total.astype(jnp.bfloat16).astype(jnp.float32)
                    new[r, c], mo[r, c], vo[r, c] = adamw(old[r, c].astype(jnp.float32), m[r, c], v[r, c], g)
                local, far = result_copies(w, q)
                for copy in (*far, *local):
                    copy.start()

        def drain_result(w, q):
            local, far = result_copies(w, q)
            for copy in local:
                copy.wait()
            for copy in far:
                copy.wait_send()

        def pass_on(i, k, o):
            w, q = at(i, k, gather_lag(o, z))

            @pl.when(valid(q))
            def _():
                pass_wait(w, q, o)

                @pl.when(q >= GAT)
                def _():
                    for copy in pass_copies(w, q - GAT, o):
                        copy.wait_send()

                for copy in pass_copies(w, q, o):
                    copy.start()

        last = WEIGHTS * PIECES + max(gather_lag(o, z) for o in range(CHIPS))

        @pl.loop(-((AHEAD + WEIGHTS - 1) // WEIGHTS), -(-last // WEIGHTS))
        def _(i):
            for k in range(WEIGHTS):
                fetch(i, k)
                for o in others:
                    forward(i, k, o)
                finish(i, k)
                for o in others:
                    pass_on(i, k, o)

        def tail(ring, wait):
            @pl.loop(PIECES - ring, PIECES)
            def _(q):
                for w in range(WEIGHTS):
                    wait(w, q)

        def tail_par(w, q):
            for o in range(CHIPS):
                par_copy(w, q, o).wait_send()

        def tail_sum(w, q):
            for o in others:
                sum_copy(w, q, o).wait_send()

        def tail_pass(w, q):
            for o in others:
                for copy in pass_copies(w, q, o):
                    copy.wait_send()

        tail(PAR, tail_par)
        tail(SND, tail_sum)
        tail(NEW, drain_result)
        tail(GAT, tail_pass)
        for w in range(WEIGHTS):
            half = whole[w].at[0]
            pltpu.make_async_copy(half, half, pal_recv.at[w]).wait()

    for z in range(CHIPS):

        @pl.when(chip == z)
        def _(z=z):
            body(z)


def communicate(terms, weights, m, v):
    def ring(dtype, *lead, of=WEIGHTS):
        return [pltpu.VMEM((*lead, *SHAPES[w]), dtype) for w in range(of)]

    def moments(arrays):
        return [(pltpu.VMEM if w == KEPT else jax.ShapeDtypeStruct)(a.shape, a.dtype) for w, a in enumerate(arrays)]

    dma = pltpu.SemaphoreType.DMA
    bf16, f32 = jnp.bfloat16, jnp.float32
    spaces = [pltpu.VMEM if w == KEPT else pl.ANY for w in range(WEIGHTS)]
    return pl.pallas_call(
        kernel,
        out_shape=[pltpu.VMEM(a.shape, a.dtype) for a in weights] + moments(m) + moments(v),
        in_specs=[pl.BlockSpec(memory_space=pl.ANY)] * (4 * WEIGHTS),
        out_specs=[pl.BlockSpec(memory_space=space) for space in (*[pltpu.VMEM] * WEIGHTS, *spaces, *spaces)],
        scratch_shapes=[
            *ring(bf16, CHIPS, OWN),
            *ring(bf16, CHIPS, PAR),
            *ring(bf16, CHIPS + 1, ARR),
            *ring(bf16, CHIPS, SND),
            *ring(f32, MOM),
            *ring(f32, MOM),
            *ring(bf16, MOM),
            *ring(f32, NEW, of=KEPT),
            *ring(f32, NEW, of=KEPT),
            dma((CHIPS, WEIGHTS, OWN)),
            dma((CHIPS, WEIGHTS, PAR)),
            dma((CHIPS, WEIGHTS, PAR)),
            dma((CHIPS + 1, WEIGHTS, ARR)),
            dma((CHIPS, WEIGHTS, SND)),
            dma((WEIGHTS, MOM)),
            dma((WEIGHTS, MOM)),
            dma((WEIGHTS, MOM)),
            dma((WEIGHTS, NEW)),
            dma((WEIGHTS, NEW)),
            dma((3, WEIGHTS, NEW)),
            dma((CHIPS, WEIGHTS, GAT)),
            dma((CHIPS, WEIGHTS, GAT)),
            dma((CHIPS, WEIGHTS, GAT)),
            dma((WEIGHTS,)),
        ],
        compiler_params=pltpu.CompilerParams(collective_id=0, has_side_effects=True, vmem_limit_bytes=GRANT),
        name="sum_step_gather",
    )(*terms, *weights, *m, *v)


def hand_out(arrays):
    kept = (0, 1, 2, 3 + KEPT, 6 + KEPT)
    rest = [n for n in range(9) if n not in kept]
    slots = 5

    def copy(*refs):
        given, out, buffer, into, out_of, sent = refs[:9], refs[9:18], *refs[18:]
        down = []
        for part in range(8):
            for n in kept:
                rows = out[n].shape[1] // 4
                where = part // 4, pl.ds(part % 4 * rows, rows)
                down.append(pltpu.make_async_copy(given[n].at[where], out[n].at[where], sent.at[n, part]))
        parts = [(n, l, pl.ds(half * 32, 32)) for n in rest for l in range(2) for half in range(2)]
        loads, stores = [], []
        for j, (n, l, rows) in enumerate(parts):
            slot = j % slots
            loads.append(pltpu.make_async_copy(given[n].at[l, rows], buffer.at[slot], into.at[slot]))
            stores.append(pltpu.make_async_copy(buffer.at[slot], out[n].at[l, rows], out_of.at[slot]))
        for load in loads[:slots]:
            load.start()
        for done in down[:8]:
            done.start()
        for j in range(len(parts)):
            loads[j].wait()
            stores[j].start()
            for done in down[8 + 2 * j : 10 + 2 * j]:
                done.start()
            if j >= 2 and j - 2 + slots < len(parts):
                stores[j - 2].wait()
                loads[j - 2 + slots].start()
        for store in stores[-slots:]:
            store.wait()
        for done in down:
            done.wait()

    dma = pltpu.SemaphoreType.DMA
    return pl.pallas_call(
        copy,
        out_shape=[jax.ShapeDtypeStruct(a.shape, a.dtype) for a in arrays],
        in_specs=[pl.BlockSpec(memory_space=pl.ANY)] * 9,
        out_specs=[pl.BlockSpec(memory_space=pl.ANY)] * 9,
        scratch_shapes=[pltpu.VMEM((slots, 32, 8192), jnp.float32), dma((slots,)), dma((slots,)), dma((9, 8))],
        compiler_params=pltpu.CompilerParams(vmem_limit_bytes=GRANT),
        name="hand_out",
    )(*[pltpu.with_memory_space_constraint(a, pltpu.VMEM if n in kept else pltpu.HBM) for n, a in enumerate(arrays)])


def solution(mesh):
    def step(*arrays):
        terms, weights, m, v = (arrays[i : i + 3] for i in (0, 3, 6, 9))
        terms = [t.reshape(t.shape[1:]) for t in terms]
        return tuple(hand_out(communicate(terms, weights, m, v)))

    all_of, cut = P(None, None, None), P(None, "dp", None)
    return jax.shard_map(
        step,
        mesh=mesh,
        in_specs=(P(("rep", "dp"), None, None, None),) * 3 + (all_of,) * 3 + (cut,) * 6,
        out_specs=(P("rep", None, None),) * 3 + (P("rep", "dp", None),) * 6,
        check_vma=False,
    )
```
